128 devices in a mesh: lat: 8 (over x, core), lon: 16 (over z, y).
Axes of the slice: x: 4, y: 4, z: 4, core: 2. Of those that a mesh axis runs over, the one named last changes fastest.
Arguments:
- queries: bfloat16 [32768, 2048], P(('lat', 'lon')), may hold values from -340 to 340
- keys: bfloat16 [32768, 2048], P(('lat', 'lon')), may hold values from -12 to 12
- values: bfloat16 [32768, 2048], P(('lat', 'lon')), may hold values from -6 to 6
- partners: int32 [128, 13], P(('lat', 'lon')), may hold values from -1 to 127, as said below
- out_weight: bfloat16 [2048, 2048], P(None, 'lat'), may hold values from -0.125 to 0.125
Outputs:
- projected: bfloat16 [32768, 2048], P(('lat', 'lon'))
The draws below stay inside these ranges and needn't reach their ends.
Inputs may be any that keep to these rules, and one draw needn't show every extreme that they name: `partners`: for each block, the first entries of its row are distinct blocks of its own band, none in its own sector or the two sectors beside it; the remaining entries are -1. In every band some block uses all 13 slots.
All inputs are finite; a program needn't handle non-finite values.
Results may differ from the reference program's by a relative error of at most 0.0095.
Values may be sent and summed in bfloat16 or wider, within the bound.
A program may use at most 128 MiB of HBM per device.

```python
import math
import jax
import jax.numpy as jnp
from jax import lax

HEADS = 16
HEAD_DIM = 128
BLOCK = 256
D = 2048
SLOTS = 13
TOKENS = 32768
N_LAT = 8
N_LON = 16


def joint_draw(key):
    block_total = N_LAT * N_LON
    key_q, key_k = jax.random.split(jax.random.fold_in(key, 7), 2)
    draw_shape = (block_total, BLOCK, HEADS, HEAD_DIM)
    query_field = jax.random.truncated_normal(key_q, -6.0, 6.0, draw_shape, jnp.float32)
    key_field = jax.random.truncated_normal(key_k, -6.0, 6.0, draw_shape, jnp.float32)
    query_field = query_field.reshape(block_total * BLOCK, HEADS * HEAD_DIM)
    key_field = key_field.reshape(block_total * BLOCK, HEADS * HEAD_DIM)
    return (query_field, key_field)


def draw_queries(key, part):
    return joint_draw(key)[0].astype(jnp.bfloat16)


def draw_keys(key, part):
    return joint_draw(key)[1].astype(jnp.bfloat16)


def draw_partners(key, part):
    block_total = N_LAT * N_LON
    key_a, key_b, key_full, key_perm = jax.random.split(jax.random.fold_in(key, 13), 4)
    first_draw = jax.random.randint(key_a, (block_total,), 1, SLOTS + 1)
    second_draw = jax.random.randint(key_b, (block_total,), 1, SLOTS + 1)
    listed_count = jnp.minimum(first_draw, second_draw)
    full_sector = jax.random.randint(key_full, (N_LAT,), 0, N_LON)
    block_ids = jnp.arange(block_total)
    band_ids = block_ids // N_LON
    sector_ids = block_ids % N_LON
    listed_count = jnp.where(sector_ids == full_sector[band_ids], SLOTS, listed_count)
    subkeys = jax.random.split(key_perm, block_total)
    offsets = jax.vmap(lambda subkey: jax.random.permutation(subkey, SLOTS))(subkeys) + 2
    chosen = band_ids[:, None] * N_LON + (sector_ids[:, None] + offsets) % N_LON
    used = jnp.arange(SLOTS)[None, :] < listed_count[:, None]
    return jnp.where(used, chosen, -1).astype(jnp.int32)


def block_levels(own_key, extent, shards, least, high):
    level = 1.0
    for dim, parts in shards:
        draws = jax.random.uniform(jax.random.fold_in(jax.random.fold_in(own_key, 6), dim), (parts,), jnp.float32, least / len(shards), high / len(shards))
        level = level * jnp.repeat(jnp.exp(draws), extent[dim] // parts).reshape((-1,) + (1,) * (len(extent) - 1 - dim))
    return level


def scatter_about(rng, dims, deviation, most, shards=(), held_as=jnp.bfloat16):
    entries = deviation * jax.random.normal(rng, dims, jnp.float32)
    if shards:
        entries = entries * block_levels(rng, dims, shards, -0.22, 0.18)
    return jnp.clip(entries, -most, most).astype(held_as)


def setup_inputs(seed: int = 0) -> dict:
    seeds = jax.random.split(jax.random.key(seed), 6)
    return {
        "queries": draw_queries(jax.random.fold_in(seeds[5], 71), 0),
        "keys": draw_keys(jax.random.fold_in(seeds[5], 71), 0),
        "values": scatter_about(seeds[2], (TOKENS, D), 1.0, 6.0, ((0, 128),)),
        "partners": draw_partners(jax.random.fold_in(seeds[5], 71), 0),
        "out_weight": scatter_about(seeds[4], (D, D), D ** -0.5, 0.125, ((1, 8),)),
    }


very_low = -1e+30

def reference(queries, keys, values, partners, out_weight):
    block_total = N_LAT * N_LON
    score_scale = 1.0 / math.sqrt(HEAD_DIM)
    query_blocks = queries.reshape(block_total, BLOCK, HEADS, HEAD_DIM)
    key_bands = keys.reshape(N_LAT, N_LON * BLOCK, HEADS, HEAD_DIM)
    value_bands = values.reshape(N_LAT, N_LON * BLOCK, HEADS, HEAD_DIM)
    sectors = jnp.arange(N_LON, dtype=jnp.int32)

    def one_block(block_id):
        band_id = block_id // N_LON
        sector = block_id % N_LON
        listed_row = lax.dynamic_index_in_dim(partners, block_id, 0, keepdims=False)
        nearby = (sectors == sector) | (sectors == (sector + 1) % N_LON) | (sectors == (sector + N_LON - 1) % N_LON)
        named = jnp.any(listed_row[:, None] - band_id * N_LON == sectors[None, :], axis=0)
        member = jnp.repeat(nearby | named, BLOCK, total_repeat_length=N_LON * BLOCK)
        query_block = lax.dynamic_index_in_dim(query_blocks, block_id, 0, keepdims=False).astype(jnp.float32)
        key_band = lax.dynamic_index_in_dim(key_bands, band_id, 0, keepdims=False).astype(jnp.float32)
        value_band = lax.dynamic_index_in_dim(value_bands, band_id, 0, keepdims=False).astype(jnp.float32)
        scores = jnp.einsum('qhd,khd->hqk', query_block, key_band) * score_scale
        scores = jnp.where(member[None, None, :], scores, very_low)
        row_max = lax.optimization_barrier(jnp.max(scores, axis=-1, keepdims=True))
        weights = jnp.exp(scores - row_max)
        row_total = lax.optimization_barrier(jnp.sum(weights, axis=-1))
        rounded = weights.astype(jnp.bfloat16).astype(jnp.float32)
        mixture = jnp.einsum('hqk,khd->qhd', rounded, value_band)
        attended = mixture / row_total.T[:, :, None]
        return attended.reshape(BLOCK, HEADS * HEAD_DIM).astype(jnp.bfloat16)
    attended = lax.map(one_block, jnp.arange(block_total, dtype=jnp.int32))
    attended = attended.reshape(block_total * BLOCK, HEADS * HEAD_DIM)
    return jnp.dot(attended, out_weight, preferred_element_type=jnp.float32).astype(jnp.bfloat16)
```

```python
import math

import jax
import jax.numpy as jnp
from jax import lax
from jax.experimental import pallas as pl
from jax.experimental.pallas import tpu as pltpu
from jax.sharding import PartitionSpec as P

NB = 16
BLK = 256
HD = 128
VR = 144
LOG2E = 1.4426950408889634

def prep_q(q):
    x = q.astype(jnp.float32) * (LOG2E / math.sqrt(HD))
    hi = x.astype(jnp.bfloat16)
    lo = (x - hi.astype(jnp.float32)).astype(jnp.bfloat16)
    return jnp.concatenate([hi, lo], axis=1)

def attn_kernel(p_ref, q_ref, k_ref, v_ref, o_ref, ti, tk, tv, qx, vt, m_ref, acc, sa, sb):
    for b in range(NB):
        qx[b] = prep_q(q_ref[b])
        vt[b, 0:HD, :] = v_ref[b].T
        row = lax.broadcasted_iota(jnp.int32, (VR - HD, BLK), 0)
        vt[b, HD:VR, :] = jnp.where(row == 0, 1.0, 0.0).astype(jnp.bfloat16)
    vt[NB] = jnp.zeros((VR, BLK), jnp.bfloat16)
    m_ref[...] = jnp.full(m_ref.shape, -1e30, jnp.float32)
    acc[...] = jnp.zeros(acc.shape, jnp.float32)

    def put(t, i, k0, k1, v1):
        ti[t] = i
        tk[2 * t] = k0
        tk[2 * t + 1] = k1
        tv[t] = v1

    def rows(i, t):
        up = lax.rem(i + 1, NB)
        down = lax.rem(i + NB - 1, NB)
        put(t, i, i, up, up)
        p0 = p_ref[i, 0]
        more = p0 >= 0
        put(t + 1, i, down, jnp.where(more, p0, down), jnp.where(more, p0, NB))
        t = t + 2
        n = jnp.int32(0)
        for s in range(1, 13):
            n = n + jnp.where(p_ref[i, s] >= 0, 1, 0)

        def pair(c, t):
            a = p_ref[i, 1 + 2 * c]
            b = p_ref[i, 2 + 2 * c]
            more = b >= 0
            put(t, i, a, jnp.where(more, b, a), jnp.where(more, b, NB))
            return t + 1
        return lax.fori_loop(0, (n + 1) // 2, pair, t)

    T = lax.fori_loop(0, NB, rows, jnp.int32(0))
    for e in range(8):
        ti[T + e] = NB
        tk[2 * (T + e)] = 0
        tk[2 * (T + e) + 1] = 0
        tv[T + e] = NB

    def scores(t, buf, slot):
        i = jnp.minimum(ti[t], NB - 1)
        k = jnp.concatenate([k_ref[tk[2 * t]], k_ref[tk[2 * t + 1]]], axis=0)
        k2 = jnp.concatenate([k, k], axis=1)
        buf[slot] = lax.dot_general(k2, qx[i], (((1,), (1,)), ((), ())), preferred_element_type=jnp.float32)

    def work(t, buf, slot):
        i = ti[t]
        s = buf[slot]
        top = jnp.max(s.reshape(2 * BLK // 8, 8, BLK), axis=0)
        top = jnp.max(top, axis=0, keepdims=True)
        old = m_ref[i]
        new = jnp.maximum(old, top)
        m_ref[i] = new
        shrink = jnp.exp2(old - new)
        w = jnp.exp2(s - new).astype(jnp.bfloat16)
        v0 = jnp.where(i == NB, NB, tk[2 * t])
        vv = jnp.concatenate([vt[v0], vt[tv[t]]], axis=1)
        part = lax.dot_general(vv, w, (((1,), (0,)), ((), ())), preferred_element_type=jnp.float32)
        acc[i] = acc[i] * shrink + part

    for u in range(2):
        scores(u, sa, u)

    def group(h, _):
        t = 4 * h
        for u in range(2):
            scores(t + 2 + u, sb, u)
        for u in range(2):
            work(t + u, sa, u)
        for u in range(2):
            scores(t + 4 + u, sa, u)
        for u in range(2):
            work(t + 2 + u, sb, u)
        return 0
    lax.fori_loop(0, (T + 3) // 4, group, 0)

    for b in range(NB):
        total = acc[b, HD:HD + 1, :]
        o_ref[b] = (acc[b, 0:HD, :] / total).astype(jnp.bfloat16)

def attention(p, q, k, v):
    NT = 16 * 8 + 8
    return pl.pallas_call(
        attn_kernel,
        out_shape=jax.ShapeDtypeStruct((NB, HD, BLK), jnp.bfloat16),
        in_specs=[pl.BlockSpec(memory_space=pltpu.SMEM)] + [pl.BlockSpec(memory_space=pltpu.VMEM)] * 3,
        out_specs=pl.BlockSpec(memory_space=pltpu.VMEM),
        scratch_shapes=[
            pltpu.SMEM((NT,), jnp.int32), pltpu.SMEM((2 * NT,), jnp.int32), pltpu.SMEM((NT,), jnp.int32),
            pltpu.VMEM((NB, BLK, 2 * HD), jnp.bfloat16),
            pltpu.VMEM((NB + 1, VR, BLK), jnp.bfloat16),
            pltpu.VMEM((NB + 1, 1, BLK), jnp.float32),
            pltpu.VMEM((NB + 1, VR, BLK), jnp.float32),
            pltpu.VMEM((2, 2 * BLK, BLK), jnp.float32),
            pltpu.VMEM((2, 2 * BLK, BLK), jnp.float32),
        ],
        name="attention",
        compiler_params=pltpu.CompilerParams(vmem_limit_bytes=40 * 1024 * 1024),
    )(p, q, k, v)

def per_device(queries, keys, values, partners, out_weight):
    band_start = lax.axis_index("lat") * NB
    heads = [a.reshape(BLK, NB, HD).transpose(1, 0, 2) for a in (queries, keys, values)]
    packed = lax.all_to_all(jnp.concatenate(heads, axis=1), "lon", 0, 0, tiled=True)
    listed = lax.all_gather(partners, "lon", axis=0, tiled=True)
    listed = jnp.where(listed >= 0, listed - band_start, -1)
    q, k, v = (packed[:, n * BLK : (n + 1) * BLK] for n in range(3))
    mixed = lax.all_to_all(attention(listed, q, k, v), "lon", 0, 0, tiled=True)
    weight = lax.all_gather(out_weight, "lat", axis=1, tiled=True)
    attended = mixed.reshape(NB * HD, BLK)
    projected = lax.dot_general(
        attended, weight, (((0,), (0,)), ((), ())), preferred_element_type=jnp.float32
    )
    return projected.astype(jnp.bfloat16)


def solution(mesh):
    return jax.shard_map(
        per_device,
        mesh=mesh,
        in_specs=(
            P(("lat", "lon"), None),
            P(("lat", "lon"), None),
            P(("lat", "lon"), None),
            P(("lat", "lon"), None),
            P(None, "lat"),
        ),
        out_specs=P(("lat", "lon"), None),
        check_vma=False,
    )
```

```python
import math

import jax
import jax.numpy as jnp
from jax import lax
from jax.experimental import pallas as pl
from jax.experimental.pallas import tpu as pltpu
from jax.sharding import PartitionSpec as P

NB = 16
BLK = 256
HD = 128
VR = 144
LOG2E = 1.4426950408889634

def prep_q(q):
    x = q.astype(jnp.float32) * (LOG2E / math.sqrt(HD))
    hi = x.astype(jnp.bfloat16)
    lo = (x - hi.astype(jnp.float32)).astype(jnp.bfloat16)
    return jnp.concatenate([hi, lo], axis=1)

def attn_kernel(p_ref, x_ref, o_ref, ti, tk, tv, qx, vt, m_ref, acc, sa, sb):
    for b in range(NB):
        qx[b] = prep_q(x_ref[b, 0])
        vt[b, 0:HD, :] = x_ref[b, 2].T
        row = lax.broadcasted_iota(jnp.int32, (VR - HD, BLK), 0)
        vt[b, HD:VR, :] = jnp.where(row == 0, 1.0, 0.0).astype(jnp.bfloat16)
    vt[NB] = jnp.zeros((VR, BLK), jnp.bfloat16)
    m_ref[...] = jnp.full(m_ref.shape, -1e30, jnp.float32)
    acc[...] = jnp.zeros(acc.shape, jnp.float32)

    def put(t, i, k0, k1, v1):
        ti[t] = i
        tk[2 * t] = k0
        tk[2 * t + 1] = k1
        tv[t] = v1

    def rows(i, t):
        up = lax.rem(i + 1, NB)
        down = lax.rem(i + NB - 1, NB)
        put(t, i, i, up, up)
        p0 = p_ref[i, 0]
        more = p0 >= 0
        put(t + 1, i, down, jnp.where(more, p0, down), jnp.where(more, p0, NB))
        t = t + 2
        n = jnp.int32(0)
        for s in range(1, 13):
            n = n + jnp.where(p_ref[i, s] >= 0, 1, 0)

        def pair(c, t):
            a = p_ref[i, 1 + 2 * c]
            b = p_ref[i, 2 + 2 * c]
            more = b >= 0
            put(t, i, a, jnp.where(more, b, a), jnp.where(more, b, NB))
            return t + 1
        return lax.fori_loop(0, (n + 1) // 2, pair, t)

    T = lax.fori_loop(0, NB, rows, jnp.int32(0))
    for e in range(8):
        ti[T + e] = NB
        tk[2 * (T + e)] = 0
        tk[2 * (T + e) + 1] = 0
        tv[T + e] = NB

    def scores(t, buf, slot):
        i = jnp.minimum(ti[t], NB - 1)
        k = jnp.concatenate([x_ref[tk[2 * t], 1], x_ref[tk[2 * t + 1], 1]], axis=0)
        k2 = jnp.concatenate([k, k], axis=1)
        buf[slot] = lax.dot_general(k2, qx[i], (((1,), (1,)), ((), ())), preferred_element_type=jnp.float32)

    def work(t, buf, slot):
        i = ti[t]
        s = buf[slot]
        top = jnp.max(s.reshape(2 * BLK // 8, 8, BLK), axis=0)
        top = jnp.max(top, axis=0, keepdims=True)
        old = m_ref[i]
        new = jnp.maximum(old, top)
        m_ref[i] = new
        shrink = jnp.exp2(old - new)
        w = jnp.exp2(s - new).astype(jnp.bfloat16)
        v0 = jnp.where(i == NB, NB, tk[2 * t])
        vv = jnp.concatenate([vt[v0], vt[tv[t]]], axis=1)
        part = lax.dot_general(vv, w, (((1,), (0,)), ((), ())), preferred_element_type=jnp.float32)
        acc[i] = acc[i] * shrink + part

    for u in range(2):
        scores(u, sa, u)

    def group(h, _):
        t = 4 * h
        for u in range(2):
            scores(t + 2 + u, sb, u)
        for u in range(2):
            work(t + u, sa, u)
        for u in range(2):
            scores(t + 4 + u, sa, u)
        for u in range(2):
            work(t + 2 + u, sb, u)
        return 0
    lax.fori_loop(0, (T + 3) // 4, group, 0)

    for b in range(NB):
        total = acc[b, HD:HD + 1, :]
        o_ref[b] = (acc[b, 0:HD, :] / total).astype(jnp.bfloat16)

def attention(p, x):
    NT = 16 * 8 + 8
    return pl.pallas_call(
        attn_kernel,
        out_shape=jax.ShapeDtypeStruct((NB, HD, BLK), jnp.bfloat16),
        in_specs=[pl.BlockSpec(memory_space=pltpu.SMEM), pl.BlockSpec(memory_space=pltpu.VMEM)],
        out_specs=pl.BlockSpec(memory_space=pltpu.VMEM),
        scratch_shapes=[
            pltpu.SMEM((NT,), jnp.int32), pltpu.SMEM((2 * NT,), jnp.int32), pltpu.SMEM((NT,), jnp.int32),
            pltpu.VMEM((NB, BLK, 2 * HD), jnp.bfloat16),
            pltpu.VMEM((NB + 1, VR, BLK), jnp.bfloat16),
            pltpu.VMEM((NB + 1, 1, BLK), jnp.float32),
            pltpu.VMEM((NB + 1, VR, BLK), jnp.float32),
            pltpu.VMEM((2, 2 * BLK, BLK), jnp.float32),
            pltpu.VMEM((2, 2 * BLK, BLK), jnp.float32),
        ],
        name="attention",
        compiler_params=pltpu.CompilerParams(vmem_limit_bytes=40 * 1024 * 1024),
    )(p, x)

MESH = pl.DeviceIdType.MESH


def wrap(a, d):
    return lax.rem(a + d, 4)


class Place:
    def __init__(self):
        lat, lon = lax.axis_index("lat"), lax.axis_index("lon")
        self.x, self.core, self.z, self.y = lat // 2, lax.rem(lat, 2), lon // 4, lax.rem(lon, 4)
        self.lat, self.lon = lat, lon

    def at(self, dx, dc, dz, dy):
        return (
            wrap(self.x, dx) * 2 + lax.rem(self.core + dc, 2),
            wrap(self.z, dz) * 4 + wrap(self.y, dy),
        )


def greet(place, peers):
    bar = pltpu.get_barrier_semaphore()
    for p in peers:
        pl.semaphore_signal(bar, inc=1, device_id=place.at(*p), device_id_type=MESH)
    pl.semaphore_wait(bar, len(peers))


def remote(src, dst, ss, rs, to):
    return pltpu.make_async_remote_copy(
        src_ref=src, dst_ref=dst, send_sem=ss, recv_sem=rs, device_id=to, device_id_type=MESH
    )


def arrived(buf, sem):
    pltpu.make_async_copy(buf, buf, sem).wait()


DIST = (1, 3, 2)
RING = [(0, 0, dz, dy) for dz in range(4) for dy in range(4) if dz or dy]


class Exchange:
    def __init__(self, place, pieces, landing, together, mid, sems):
        self.place, self.pieces, self.landing, self.together = place, pieces, landing, together
        self.mid = mid
        self.s1, self.r1, self.s2, self.r2 = sems

    def passing(self, half, d, g, n):
        slot = self.mid.at[half, d - 1, g - 1]
        return slot.at[n] if len(slot.shape) == 3 else slot

    def along(self, half, first, second):
        return (second, first) if half == 0 else (first, second)

    def lon_at(self, dz, dy):
        return wrap(self.place.z, dz) * 4 + wrap(self.place.y, dy)

    def first_leg(self):
        me = self.place.lon
        for d in DIST:
            for g in range(4):
                for half in range(2):
                    to = self.place.at(0, 0, *self.along(half, d, 0))
                    head = self.lon_at(*self.along(half, d, g))
                    k = min(g, 1)
                    land = self.landing(half, me)
                    for n, src in enumerate(self.pieces(half, head)):
                        dst = land[n] if g == 0 else self.passing(half, d, g, n)
                        remote(src, dst, self.s1.at[half, d - 1, k], self.r1.at[half, d - 1, k], to).start()

    def second_leg_own(self):
        me = self.place.lon
        for g in DIST:
            for half in range(2):
                dz, dy = self.along(half, 0, g)
                land = self.landing(half, me)
                for n, src in enumerate(self.pieces(half, self.lon_at(dz, dy))):
                    remote(src, land[n], self.s2.at[half, g - 1, 0], self.r2.at[half, g - 1, 0],
                           self.place.at(0, 0, dz, dy)).start()

    def pass_on(self):
        for d in DIST:
            for half in range(2):
                arrived(self.mid.at[half, d - 1], self.r1.at[half, d - 1, 1])
                block = self.lon_at(*self.along(half, 4 - d, 0))
                for g in DIST:
                    to = self.place.at(0, 0, *self.along(half, 0, g))
                    remote(self.mid.at[half, d - 1, g - 1], self.together(half, block),
                           self.s2.at[half, g - 1, d], self.r2.at[half, g - 1, d], to).start()

    def finish(self):
        for half in range(2):
            one = self.together(half, 0)
            for d in DIST:
                arrived(one, self.r1.at[half, d - 1, 0])
                arrived(one, self.s1.at[half, d - 1, 0])
                arrived(self.mid.at[half, d - 1], self.s1.at[half, d - 1, 1])
                for g in range(4):
                    arrived(one, self.r2.at[half, d - 1, g])
                    arrived(one, self.s2.at[half, d - 1, g])


EXCHANGE_SEMS = [pltpu.SemaphoreType.DMA(s) for s in ((2, 3, 2), (2, 3, 2), (2, 3, 4), (2, 3, 4))]


def scatter_kernel(q, k, v, w, p, xo, wo, po, mid, s1, r1, s2, r2, ws, wr, ps, pr, lsem):
    place = Place()
    lat, lon = place.lat, place.lon
    greet(place, RING + [(1, 0, 0, 0), (3, 0, 0, 0), (0, 1, 0, 0)])
    rows = (pl.ds(0, BLK // 2), pl.ds(BLK // 2, BLK // 2))
    col = lambda h: pl.ds(pl.multiple_of(h * HD, HD), HD)
    started = []
    for n, o in enumerate(RING):
        c = remote(p, po.at[lon], ps.at[n], pr.at[n], place.at(*o))
        c.start()
        started.append(c)
    local = [pltpu.make_async_copy(a.at[:, col(lon)], xo.at[lon, n], lsem.at[n]) for n, a in enumerate((q, k, v))]
    local += [pltpu.make_async_copy(w, wo.at[lat], lsem.at[3]), pltpu.make_async_copy(p, po.at[lon], lsem.at[4])]
    for c in local:
        c.start()
    ex = Exchange(
        place,
        lambda half, head: [a.at[rows[half], col(head)] for a in (q, k, v)],
        lambda half, block: [xo.at[block, n, rows[half]] for n in range(3)],
        lambda half, block: xo.at[block, :, rows[half]],
        mid, (s1, r1, s2, r2),
    )

    def send_w(src, n, to):
        c = remote(src, src, ws.at[n], wr.at[n], to)
        c.start()
        started.append(c)

    own = remote(w, wo.at[lat], ws.at[0], wr.at[0], place.at(1, 0, 0, 0))
    back = remote(w, wo.at[lat], ws.at[1], wr.at[1], place.at(3, 0, 0, 0))
    side = remote(w, wo.at[lat], ws.at[2], wr.at[2], place.at(0, 1, 0, 0))
    for c in (own, back, side):
        c.start()
        started.append(c)
    ex.first_leg()
    ex.second_leg_own()
    ex.pass_on()
    left, right, far = (wrap(place.x, d) * 2 + place.core for d in (3, 1, 2))
    top, low = pl.ds(0, 1024), pl.ds(1024, 1024)
    arrived(wo.at[left], wr.at[0])
    send_w(wo.at[left, top], 3, place.at(1, 0, 0, 0))
    send_w(wo.at[left], 4, place.at(0, 1, 0, 0))
    arrived(wo.at[right], wr.at[1])
    send_w(wo.at[right, low], 5, place.at(3, 0, 0, 0))
    send_w(wo.at[right], 6, place.at(0, 1, 0, 0))
    arrived(wo.at[far, top], wr.at[3])
    send_w(wo.at[far, top], 7, place.at(0, 1, 0, 0))
    arrived(wo.at[far, low], wr.at[5])
    send_w(wo.at[far, low], 8, place.at(0, 1, 0, 0))
    ex.finish()
    for c in local:
        c.wait()
    for c in started:
        c.wait_send()
    for n in range(len(RING)):
        arrived(po.at[0], pr.at[n])
    for n in (2, 4, 6):
        arrived(wo.at[0], wr.at[n])
    for n in (7, 8):
        arrived(wo.at[0, top], wr.at[n])


def scatter(q, k, v, w, p):
    anywhere, vmem = pl.BlockSpec(memory_space=pl.ANY), pl.BlockSpec(memory_space=pltpu.VMEM)
    DMA = pltpu.SemaphoreType.DMA
    return pl.pallas_call(
        scatter_kernel,
        out_shape=(
            jax.ShapeDtypeStruct((NB, 3, BLK, HD), jnp.bfloat16),
            jax.ShapeDtypeStruct((8, 2048, 256), jnp.bfloat16),
            jax.ShapeDtypeStruct((NB, 8, 128), jnp.int32),
        ),
        in_specs=[anywhere] * 4 + [vmem],
        out_specs=(vmem, anywhere, vmem),
        scratch_shapes=[pltpu.VMEM((2, 3, 3, 3, BLK // 2, HD), jnp.bfloat16)]
        + EXCHANGE_SEMS
        + [DMA((9,)), DMA((9,)), DMA((15,)), DMA((15,)), DMA((5,))],
        name="scatter_heads",
        compiler_params=pltpu.CompilerParams(
            collective_id=0, has_side_effects=True, vmem_limit_bytes=32 * 1024 * 1024
        ),
    )(q, k, v, w, p)


def gather_kernel(o_ref, w_ref, out_ref, land, att, mid, s1, r1, s2, r2, lsem):
    place = Place()
    greet(place, [o for o in RING if not (o[2] and o[3])])
    rows = (pl.ds(0, HD // 2), pl.ds(HD // 2, HD // 2))
    own = pltpu.make_async_copy(o_ref.at[place.lon], land.at[place.lon], lsem)
    own.start()
    ex = Exchange(
        place,
        lambda half, head: [o_ref.at[head, rows[half]]],
        lambda half, block: [land.at[block, rows[half]]],
        lambda half, block: land.at[block, rows[half]],
        mid, (s1, r1, s2, r2),
    )
    ex.first_leg()
    ex.second_leg_own()
    ex.pass_on()
    ex.finish()
    own.wait()
    for h in range(NB):
        att[:, h * HD:(h + 1) * HD] = land[h].T

    def tile(n, _):
        out_ref[:, pl.ds(pl.multiple_of(n * 256, 256), 256)] = jnp.dot(
            att[...], w_ref[n], preferred_element_type=jnp.float32
        ).astype(jnp.bfloat16)
        return 0
    lax.fori_loop(0, 8, tile, 0)


def gather_project(o, w):
    vmem = pl.BlockSpec(memory_space=pltpu.VMEM)
    return pl.pallas_call(
        gather_kernel,
        out_shape=jax.ShapeDtypeStruct((BLK, 2048), jnp.bfloat16),
        in_specs=[pl.BlockSpec(memory_space=pl.ANY), vmem],
        out_specs=vmem,
        scratch_shapes=[
            pltpu.VMEM((NB, HD, BLK), jnp.bfloat16),
            pltpu.VMEM((BLK, 2048), jnp.bfloat16),
            pltpu.VMEM((2, 3, 3, HD // 2, BLK), jnp.bfloat16),
        ]
        + EXCHANGE_SEMS
        + [pltpu.SemaphoreType.DMA],
        name="gather_project",
        compiler_params=pltpu.CompilerParams(
            collective_id=1, has_side_effects=True, vmem_limit_bytes=32 * 1024 * 1024
        ),
    )(o, w)


def per_device(queries, keys, values, partners, out_weight):
    band_start = lax.axis_index("lat") * NB
    listed = jnp.where(partners >= 0, partners - band_start, -1)
    listed = jnp.pad(listed, ((0, 7), (0, 128 - listed.shape[1])), constant_values=-1)
    packed, weight, listed = scatter(queries, keys, values, out_weight, listed)
    return gather_project(attention(listed[:, 0, :13], packed), weight)


def solution(mesh):
    return jax.shard_map(
        per_device,
        mesh=mesh,
        in_specs=(
            P(("lat", "lon"), None),
            P(("lat", "lon"), None),
            P(("lat", "lon"), None),
            P(("lat", "lon"), None),
            P(None, "lat"),
        ),
        out_specs=P(("lat", "lon"), None),
        check_vma=False,
    )
```

```python
import math

import jax
import jax.numpy as jnp
from jax import lax
from jax.experimental import pallas as pl
from jax.experimental.pallas import tpu as pltpu
from jax.sharding import PartitionSpec as P

NB = 16
BLK = 256
HALF = BLK // 2
HD = 128
VR = 144
D = 2048
SCALE = math.log2(math.e) / math.sqrt(HD)
LOW = -1e30


def split_q(q):
    x = q.astype(jnp.float32) * SCALE
    high = x.astype(jnp.bfloat16)
    low = (x - high.astype(jnp.float32)).astype(jnp.bfloat16)
    return jnp.concatenate([high, low], axis=1)


def bias_of(row, block):
    j = lax.broadcasted_iota(jnp.int32, (NB, HALF), 0)
    named = jnp.max(jnp.where(row == j, 1.0, 0.0), axis=1, keepdims=True) > 0.5
    near = (j == block) | (j == lax.rem(block + 1, NB)) | (j == lax.rem(block + NB - 1, NB))
    return jnp.where(named | near, 0.0, LOW)


CHUNK = 2


def scores(qx, bias, k_ref, s_ref, sub_ref):
    best = None
    for c in range(0, NB, CHUNK):
        keys = k_ref[c:c + CHUNK].reshape(CHUNK * BLK, HD)
        s = lax.dot_general(
            jnp.concatenate([keys, keys], axis=1), qx, (((1,), (1,)), ((), ())),
            preferred_element_type=jnp.float32,
        )
        s_ref[c * BLK:(c + CHUNK) * BLK, :] = s
        for j in range(CHUNK):
            part = jnp.max(s[j * BLK:(j + 1) * BLK].reshape(BLK // 8, 8, BLK), axis=0)
            part = part + bias[c + j:c + j + 1, :]
            best = part if best is None else jnp.maximum(best, part)
    sub_ref[...] = jnp.max(best, axis=0, keepdims=True) - bias


def mix(s_ref, sub_ref, vt_ref):
    total = None
    for c in range(0, NB, CHUNK):
        w = [
            jnp.exp2(s_ref[j * BLK:(j + 1) * BLK, :] - sub_ref[j:j + 1, :]).astype(jnp.bfloat16)
            for j in range(c, c + CHUNK)
        ]
        part = jnp.dot(
            vt_ref[:, c * BLK:(c + CHUNK) * BLK], jnp.concatenate(w, axis=0),
            preferred_element_type=jnp.float32,
        )
        total = part if total is None else total + part
    return (total[0:HD] / total[HD:HD + 1]).astype(jnp.bfloat16)


MESH = pl.DeviceIdType.MESH
DIST = (1, 3, 2)
RING = [(0, 0, dz, dy) for dz in range(4) for dy in range(4) if dz or dy]
UNITS = [(0, 0), (1, 0), (3, 0), (2, 0), (0, 1), (0, 3), (0, 2)]
UNITS += [(1, 1), (1, 3), (3, 1), (3, 3), (2, 2), (1, 2), (2, 1), (3, 2), (2, 3)]
EARLY = 12


def wrap(a, d):
    return lax.rem(a + d, 4)


def back(d):
    return (4 - d) % 4


def ds128(i, n=1):
    return pl.ds(pl.multiple_of(i * 128, 128), n * 128)


class Place:
    def __init__(self):
        lat, lon = lax.axis_index("lat"), lax.axis_index("lon")
        self.x, self.core, self.z, self.y = lat // 2, lax.rem(lat, 2), lon // 4, lax.rem(lon, 4)
        self.lat, self.lon = lat, lon

    def at(self, dx, dc, dz, dy):
        return (
            wrap(self.x, dx) * 2 + lax.rem(self.core + dc, 2),
            wrap(self.z, dz) * 4 + wrap(self.y, dy),
        )

    def lon_at(self, dz, dy):
        return wrap(self.z, dz) * 4 + wrap(self.y, dy)


def remote(src, dst, ss, rs, to):
    return pltpu.make_async_remote_copy(
        src_ref=src, dst_ref=dst, send_sem=ss, recv_sem=rs, device_id=to, device_id_type=MESH
    )


def arrived(buf, sem):
    pltpu.make_async_copy(buf, buf, sem).wait()


def along(half, first, second):
    return (second, first) if half == 0 else (first, second)


class Exchange:
    def __init__(self, place, piece, landing, mid, s1, r1, s2, r2):
        self.place, self.piece, self.landing, self.mid = place, piece, landing, mid
        self.s1, self.r1, self.s2, self.r2 = s1, r1, s2, r2

    def start(self):
        place = self.place
        for d in DIST:
            for g in (0, 1, 3, 2):
                for half in range(2):
                    to = place.at(0, 0, *along(half, d, 0))
                    src = self.piece(half, place.lon_at(*along(half, d, g)))
                    dst = self.mid.at[half, d - 1, g - 1] if g else self.landing(half, d, 0, place.lon)
                    k = min(g, 1)
                    remote(src, dst, self.s1.at[half, d - 1, k], self.r1.at[half, d - 1, k], to).start()
        for g in DIST:
            for half in range(2):
                o = along(half, 0, g)
                remote(
                    self.piece(half, place.lon_at(*o)), self.landing(half, 0, g, place.lon),
                    self.s2.at[half, g - 1, 0], self.r2.at[half, g - 1, 0], place.at(0, 0, *o),
                ).start()

    def pass_on(self, d):
        place = self.place
        for half in range(2):
            arrived(self.mid.at[half, d - 1], self.r1.at[half, d - 1, 1])
            block = place.lon_at(*along(half, 4 - d, 0))
            for g in DIST:
                remote(
                    self.mid.at[half, d - 1, g - 1], self.landing(half, d, g, block),
                    self.s2.at[half, g - 1, d], self.r2.at[half, g - 1, d],
                    place.at(0, 0, *along(half, 0, g)),
                ).start()

    def landed(self, half, d, g):
        block = self.place.lon_at(*along(half, back(d), back(g)))
        ref = self.landing(half, d, g, block)
        if g:
            arrived(ref, self.r2.at[half, g - 1, d])
        elif d:
            arrived(ref, self.r1.at[half, d - 1, 0])
        return block, ref

    def sent(self):
        one = self.mid.at[0, 0, 0]
        for half in range(2):
            for d in range(3):
                arrived(one, self.s1.at[half, d, 0])
                arrived(self.mid.at[half, d], self.s1.at[half, d, 1])
                for g in range(4):
                    arrived(one, self.s2.at[half, d, g])


def kernel(
    q, k, v, w, p, out,
    mine, kland, vland, qland, table, vt, sa, sb, ba, bb, osend, heads, att, partial, weight, mid,
    ks1, kr1, ks2, kr2, vs1, vr1, vs2, vr2, qs1, qr1, qs2, qr2,
    os, orr, ws, wr, ps, pr, lsem,
):
    place = Place()
    lat, lon = place.lat, place.lon
    rows = (pl.ds(0, HALF), pl.ds(HALF, HALF))
    loads = [pltpu.make_async_copy(a, mine.at[n], lsem.at[n]) for n, a in enumerate((k, v, q))]
    for c in loads:
        c.start()
    local = [
        pltpu.make_async_copy(k.at[:, ds128(lon)], kland.at[lon], lsem.at[3]),
        pltpu.make_async_copy(v.at[:, ds128(lon)], vland.at[lon], lsem.at[4]),
        pltpu.make_async_copy(q.at[:, ds128(lon)], qland.at[0], lsem.at[5]),
        pltpu.make_async_copy(w, weight.at[lat], lsem.at[6]),
        pltpu.make_async_copy(p, table.at[lon], lsem.at[7]),
    ]
    for c in local:
        c.start()

    peers = RING + [(1, 0, 0, 0), (3, 0, 0, 0), (0, 1, 0, 0)]
    bar = pltpu.get_barrier_semaphore()
    for o in peers:
        pl.semaphore_signal(bar, inc=1, device_id=place.at(*o), device_id_type=MESH)
    pl.semaphore_wait(bar, len(peers))

    started = []

    def send(*args):
        c = remote(*args)
        c.start()
        started.append(c)

    for n, o in enumerate(RING):
        send(p, table.at[lon], ps.at[n], pr.at[n], place.at(*o))

    def exchange(n, landing, *sems):
        return Exchange(
            place, lambda half, head: mine.at[n, rows[half], ds128(head)], landing, mid.at[n], *sems
        )

    ke = exchange(0, lambda half, d, g, b: kland.at[b, rows[half]], ks1, kr1, ks2, kr2)
    ve = exchange(1, lambda half, d, g, b: vland.at[b, rows[half]], vs1, vr1, vs2, vr2)
    qe = exchange(2, lambda half, d, g, b: qland.at[UNITS.index((d, g)), rows[half]], qs1, qr1, qs2, qr2)
    loads[0].wait()
    ke.start()
    send(w, weight.at[lat], ws.at[0], wr.at[0], place.at(1, 0, 0, 0))
    send(w, weight.at[lat], ws.at[1], wr.at[1], place.at(3, 0, 0, 0))
    send(w, weight.at[lat], ws.at[2], wr.at[2], place.at(0, 1, 0, 0))
    loads[1].wait()
    ve.start()
    loads[2].wait()
    for d in DIST:
        ke.pass_on(d)
    for d in DIST:
        ve.pass_on(d)
    qe.start()

    for c in local:
        c.wait()
    for n in range(len(RING)):
        arrived(table.at[0], pr.at[n])
    vt[HD:VR, :] = jnp.where(
        lax.broadcasted_iota(jnp.int32, (VR - HD, NB * BLK), 0) == 0, 1.0, 0.0
    ).astype(jnp.bfloat16)

    def turn(half, d, g):
        b, ref = ve.landed(half, d, g)
        vt[0:HD, ds128(2 * b + half)] = ref[...].T

    for half in range(2):
        for d, g in UNITS[:7]:
            turn(half, d, g)
    for d, g in UNITS[1:]:
        for half in range(2):
            ke.landed(half, d, g)

    def unit_blocks(u):
        d, g = UNITS[u]
        return [place.lon_at(*along(half, back(d), back(g))) for half in range(2)]

    S, B = (sa, sb), (ba, bb)

    def score(u):
        bias = [bias_of(table[b][0:1, :], b) for b in unit_blocks(u)]
        scores(split_q(qland[u]), jnp.concatenate(bias, axis=1), kland, S[u % 2], B[u % 2])

    score(0)
    for d, g in UNITS[7:]:
        for half in range(2):
            turn(half, d, g)

    left, right, far = (wrap(place.x, n) * 2 + place.core for n in (3, 1, 2))
    top, low = pl.ds(0, D // 2), pl.ds(D // 2, D // 2)

    def ring(src, n, to):
        send(src, src, ws.at[n], wr.at[n], to)

    def weight_step(u):
        if u == 3:
            arrived(weight.at[left], wr.at[0])
            ring(weight.at[left, top], 3, place.at(1, 0, 0, 0))
            ring(weight.at[left], 4, place.at(0, 1, 0, 0))
            arrived(weight.at[right], wr.at[1])
            ring(weight.at[right, low], 5, place.at(3, 0, 0, 0))
            ring(weight.at[right], 6, place.at(0, 1, 0, 0))
        if u == 13:
            arrived(weight.at[far, top], wr.at[3])
            ring(weight.at[far, top], 7, place.at(0, 1, 0, 0))
            arrived(weight.at[far, low], wr.at[5])
            ring(weight.at[far, low], 8, place.at(0, 1, 0, 0))

    def give_back(u):
        d, g = UNITS[u]
        if u == 0:
            return
        for half in range(2):
            dz, dy = along(half, d, g)
            lanes = pl.ds(half * HALF, HALF)
            send(
                osend.at[u, :, lanes], heads.at[UNITS.index((dz, dy)), :, lanes],
                os.at[u, half], orr.at[u, half], place.at(0, 0, back(dz), back(dy)),
            )

    for u in range(NB):
        if u < NB - 1:
            d, g = UNITS[u + 1]
            if g == 0:
                qe.pass_on(d)
            for half in range(2):
                qe.landed(half, d, g)
            score(u + 1)
        if u == 0:
            heads[0] = mix(S[0], B[0], vt)
        else:
            osend[u] = mix(S[u % 2], B[u % 2], vt)
            give_back(u - 1)
        weight_step(u)

    for n in (2, 4, 6):
        arrived(weight.at[0], wr.at[n])
    for n in (7, 8):
        arrived(weight.at[0, top], wr.at[n])

    def fetch(units):
        for u in units:
            for half in range(2):
                if u:
                    arrived(osend.at[0, :, pl.ds(0, HALF)], orr.at[u, half])
        for u in units:
            att[:, u * HD:(u + 1) * HD] = heads[u].T

    def weight_rows(units, n):
        return jnp.concatenate(
            [weight[n, ds128(place.lon_at(*UNITS[u])), :] for u in units], axis=0
        )

    give_back(NB - 1)
    fetch(range(EARLY))

    def first(n, _):
        partial[n] = jnp.dot(
            att[:, 0:EARLY * HD], weight_rows(range(EARLY), n), preferred_element_type=jnp.float32
        )
        return 0

    lax.fori_loop(0, 8, first, 0)
    fetch(range(EARLY, NB))
    for n in range(8):
        out[:, n * 256:(n + 1) * 256] = (
            partial[n]
            + jnp.dot(
                att[:, EARLY * HD:], weight_rows(range(EARLY, NB), n), preferred_element_type=jnp.float32
            )
        ).astype(jnp.bfloat16)
    for e in (ke, ve, qe):
        e.sent()
    for c in started:
        c.wait_send()


def per_device(queries, keys, values, partners, out_weight):
    band_start = lax.axis_index("lat") * NB
    listed = jnp.where(partners >= 0, partners - band_start, -1)
    listed = jnp.pad(listed, ((0, 7), (0, 128 - listed.shape[1])), constant_values=-1)
    hbm, vmem = pl.BlockSpec(memory_space=pltpu.HBM), pl.BlockSpec(memory_space=pltpu.VMEM)
    dma = pltpu.SemaphoreType.DMA
    bf16, f32 = jnp.bfloat16, jnp.float32
    return pl.pallas_call(
        kernel,
        out_shape=jax.ShapeDtypeStruct((BLK, D), bf16),
        in_specs=[hbm] * 4 + [vmem],
        out_specs=vmem,
        scratch_shapes=[
            pltpu.VMEM((3, BLK, D), bf16),
            pltpu.VMEM((NB, BLK, HD), bf16),
            pltpu.VMEM((NB, BLK, HD), bf16),
            pltpu.VMEM((NB, BLK, HD), bf16),
            pltpu.VMEM((NB, 8, 128), jnp.int32),
            pltpu.VMEM((VR, NB * BLK), bf16),
            pltpu.VMEM((NB * BLK, BLK), f32),
            pltpu.VMEM((NB * BLK, BLK), f32),
            pltpu.VMEM((NB, BLK), f32),
            pltpu.VMEM((NB, BLK), f32),
            pltpu.VMEM((NB, HD, BLK), bf16),
            pltpu.VMEM((NB, HD, BLK), bf16),
            pltpu.VMEM((BLK, D), bf16),
            pltpu.VMEM((8, BLK, 256), f32),
            pltpu.VMEM((8, D, 256), bf16),
            pltpu.VMEM((3, 2, 3, 3, HALF, HD), bf16),
        ]
        + [dma((2, 3, 2)), dma((2, 3, 2)), dma((2, 3, 4)), dma((2, 3, 4))] * 3
        + [dma((NB, 2)), dma((NB, 2)), dma((9,)), dma((9,)), dma((15,)), dma((15,)), dma((8,))],
        name="band_attention",
        compiler_params=pltpu.CompilerParams(
            collective_id=0, has_side_effects=True, vmem_limit_bytes=60 * 1024 * 1024
        ),
    )(queries, keys, values, out_weight, listed)


def solution(mesh):
    return jax.shard_map(
        per_device,
        mesh=mesh,
        in_specs=(
            P(("lat", "lon"), None),
            P(("lat", "lon"), None),
            P(("lat", "lon"), None),
            P(("lat", "lon"), None),
            P(None, "lat"),
        ),
        out_specs=P(("lat", "lon"), None),
        check_vma=False,
    )
```

```python
import math

import jax
import jax.numpy as jnp
from jax import lax
from jax.experimental import pallas as pl
from jax.experimental.pallas import tpu as pltpu
from jax.sharding import PartitionSpec as P

NB = 16
BLK = 256
HALF = BLK // 2
HD = 128
VR = 144
D = 2048
SCALE = math.log2(math.e) / math.sqrt(HD)
LOW = -1e30
SLOTS = 13


def split_q(q):
    x = q.astype(jnp.float32) * SCALE
    high = x.astype(jnp.bfloat16)
    low = (x - high.astype(jnp.float32)).astype(jnp.bfloat16)
    return jnp.concatenate([high, low], axis=1)


def bias_of(row, block, band_start):
    j = lax.broadcasted_iota(jnp.int32, (NB, SLOTS), 0)
    named = jnp.max(jnp.where(row == j + band_start, 1.0, 0.0), axis=1, keepdims=True)
    j = lax.broadcasted_iota(jnp.int32, (NB, BLK), 0)
    near = (j == block) | (j == lax.rem(block + 1, NB)) | (j == lax.rem(block + NB - 1, NB))
    return jnp.where(near, 0.0, jnp.where(named > 0.5, 0.0, LOW))


def step(s_ref, w_ref, sub_ref, vt_ref, k_ref, qx=None, bias=None, weigh=True, blend=True):
    best, total = None, None
    for j in range(NB):
        at = slice(j * BLK, (j + 1) * BLK)
        if blend:
            part = jnp.dot(vt_ref[:, at], w_ref[at, :], preferred_element_type=jnp.float32)
            total = part if total is None else total + part
        if weigh:
            less = sub_ref[j:j + 1, :]
            for r in range(j * BLK, (j + 1) * BLK, 16):
                w_ref[r:r + 16, :] = jnp.exp2(s_ref[r:r + 16, :] - less).astype(jnp.bfloat16)
        if qx is not None:
            keys = k_ref[j]
            s = lax.dot_general(
                jnp.concatenate([keys, keys], axis=1), qx, (((1,), (1,)), ((), ())),
                preferred_element_type=jnp.float32,
            )
            s_ref[at, :] = s
            part = jnp.max(s.reshape(BLK // 8, 8, BLK), axis=0) + bias[j:j + 1, :]
            best = part if best is None else jnp.maximum(best, part)
    if qx is not None:
        sub_ref[...] = jnp.max(best, axis=0, keepdims=True) - bias
    if blend:
        return (total[0:HD] / total[HD:HD + 1]).astype(jnp.bfloat16)
    return None


MESH = pl.DeviceIdType.MESH
DIST = (1, 3, 2)
RING = [(0, 0, dz, dy) for dz in range(4) for dy in range(4) if dz or dy]
EARLY = 12


def unit_at(u):
    four, seven = (u + 12) // 16, (u + 9) // 16
    dz = (four - seven) * (u - 3) + seven * ((u + 2) // 3 - 2)
    dy = (1 - four) * u + seven * ((u + 2) % 3 + 1)
    return dz, dy


UNITS = [unit_at(u) for u in range(NB)]


def wrap(a, d):
    return lax.rem(a + d, 4)


def back(d):
    return (4 - d) % 4


def ds128(i, n=1):
    return pl.ds(pl.multiple_of(i * 128, 128), n * 128)


class Place:
    def __init__(self):
        lat, lon = lax.axis_index("lat"), lax.axis_index("lon")
        self.x, self.core, self.z, self.y = lat // 2, lax.rem(lat, 2), lon // 4, lax.rem(lon, 4)
        self.lat, self.lon = lat, lon

    def at(self, dx, dc, dz, dy):
        return (
            wrap(self.x, dx) * 2 + lax.rem(self.core + dc, 2),
            wrap(self.z, dz) * 4 + wrap(self.y, dy),
        )

    def lon_at(self, dz, dy):
        return wrap(self.z, dz) * 4 + wrap(self.y, dy)


def remote(src, dst, ss, rs, to):
    return pltpu.make_async_remote_copy(
        src_ref=src, dst_ref=dst, send_sem=ss, recv_sem=rs, device_id=to, device_id_type=MESH
    )


def arrived(buf, sem):
    pltpu.make_async_copy(buf, buf, sem).wait()


def along(half, first, second):
    return (second, first) if half == 0 else (first, second)


class Exchange:
    def __init__(self, place, piece, landing, mid, sm, rm, sf, rf):
        self.place, self.piece, self.landing, self.mid = place, piece, landing, mid
        self.sm, self.rm, self.sf, self.rf = sm, rm, sf, rf

    def start_straight(self, distances=DIST):
        place = self.place
        for n in distances:
            for d, g in ((n, 0), (0, n)):
                for half in range(2):
                    o = along(half, d, g)
                    remote(
                        self.piece(half, place.lon_at(*o)), self.landing(half, d, g, place.lon),
                        self.sf.at[half, d, g], self.rf.at[half, d, g], place.at(0, 0, *o),
                    ).start()

    def start_bent(self, d):
        place = self.place
        for g in DIST:
            for half in range(2):
                remote(
                    self.piece(half, place.lon_at(*along(half, d, g))), self.mid.at[half, d - 1, g - 1],
                    self.sm.at[half, d - 1], self.rm.at[half, d - 1], place.at(0, 0, *along(half, d, 0)),
                ).start()

    def pass_on(self, d):
        place = self.place
        for half in range(2):
            arrived(self.mid.at[half, d - 1], self.rm.at[half, d - 1])
            block = place.lon_at(*along(half, back(d), 0))
            for g in DIST:
                remote(
                    self.mid.at[half, d - 1, g - 1], self.landing(half, d, g, block),
                    self.sf.at[half, d, g], self.rf.at[half, d, g], place.at(0, 0, *along(half, 0, g)),
                ).start()

    def landed(self, half, d, g):
        block = self.place.lon_at(*along(half, back(d), back(g)))
        ref = self.landing(half, d, g, block)
        if d or g:
            arrived(ref, self.rf.at[half, d, g])
        return block, ref

    def sent(self):
        one = self.mid.at[0, 0, 0]
        for half in range(2):
            for d in range(4):
                if d:
                    arrived(self.mid.at[half, d - 1], self.sm.at[half, d - 1])
                for g in range(4):
                    if d or g:
                        arrived(one, self.sf.at[half, d, g])


def kernel(
    q, k, v, w, p, out,
    mine, kland, vland, qland, table, vt, sbuf, wbuf, sub, osend, heads, att, partial, weight, mid,
    ksm, krm, ksf, krf, vsm, vrm, vsf, vrf, qsm, qrm, qsf, qrf,
    os, orr, ws, wr, ps, pr, lsem,
):
    place = Place()
    lat, lon = place.lat, place.lon
    band_start = lat * NB
    rows = (pl.ds(0, HALF), pl.ds(HALF, HALF))
    loads = [pltpu.make_async_copy(a, mine.at[n], lsem.at[n]) for n, a in enumerate((k, v, q))]
    for c in loads:
        c.start()
    local = [
        pltpu.make_async_copy(k.at[:, ds128(lon)], kland.at[lon], lsem.at[3]),
        pltpu.make_async_copy(v.at[:, ds128(lon)], vland.at[lon], lsem.at[4]),
        pltpu.make_async_copy(q.at[:, ds128(lon)], qland.at[0], lsem.at[5]),
        pltpu.make_async_copy(w, weight.at[lat], lsem.at[6]),
        pltpu.make_async_copy(p, table.at[lon], lsem.at[7]),
    ]
    for c in local:
        c.start()

    peers = RING + [(1, 0, 0, 0), (3, 0, 0, 0), (0, 1, 0, 0)]
    bar = pltpu.get_barrier_semaphore()
    with jax.named_scope("barrier"):
        for o in peers:
            pl.semaphore_signal(bar, inc=1, device_id=place.at(*o), device_id_type=MESH)
        pl.semaphore_wait(bar, len(peers))

    started = []

    def send(*args):
        c = remote(*args)
        c.start()
        started.append(c)

    for n, o in enumerate(RING):
        send(p, table.at[lon], ps.at[n], pr.at[n], place.at(*o))

    def exchange(n, landing, *sems):
        return Exchange(
            place, lambda half, head: mine.at[n, rows[half], ds128(head)], landing, mid.at[n], *sems
        )

    ke = exchange(0, lambda half, d, g, b: kland.at[b, rows[half]], ksm, krm, ksf, krf)
    ve = exchange(1, lambda half, d, g, b: vland.at[b, rows[half]], vsm, vrm, vsf, vrf)
    qe = exchange(
        2, lambda half, d, g, b: qland.at[UNITS.index(along(half, d, g)), rows[half]], qsm, qrm, qsf, qrf
    )
    with jax.named_scope("starts"):
        for n, e in enumerate((ke, ve)):
            loads[n].wait()
            for d in DIST:
                e.start_bent(d)
            e.start_straight()
            if n == 0:
                send(w, weight.at[lat], ws.at[0], wr.at[0], place.at(1, 0, 0, 0))
                send(w, weight.at[lat], ws.at[1], wr.at[1], place.at(3, 0, 0, 0))
                send(w, weight.at[lat], ws.at[2], wr.at[2], place.at(0, 1, 0, 0))
        loads[2].wait()
    with jax.named_scope("k_pass"):
        for d in DIST:
            ke.pass_on(d)
    with jax.named_scope("v_pass"):
        for d in DIST:
            ve.pass_on(d)

    with jax.named_scope("table"):
        for c in local:
            c.wait()
        for n in range(len(RING)):
            arrived(table.at[0], pr.at[n])
        vt[HD:VR, :] = jnp.where(
            lax.broadcasted_iota(jnp.int32, (VR - HD, NB * BLK), 0) == 0, 1.0, 0.0
        ).astype(jnp.bfloat16)

    def turn(half, dz, dy):
        b, ref = ve.landed(half, *along(half, dz, dy))
        vt[0:HD, ds128(2 * b + half)] = ref[...].T

    def score_args(u):
        dz, dy = unit_at(u)
        b = place.lon_at(back(dz), back(dy))
        return split_q(qland[u]), bias_of(table[b], b, band_start)

    def turn_step(**kwargs):
        return step(sbuf, wbuf, sub, vt, kland, **kwargs)

    with jax.named_scope("turn1"):
        for half in range(2):
            for dz, dy in UNITS[:7]:
                turn(half, dz, dy)
    with jax.named_scope("k_wait"):
        for dz, dy in UNITS[1:]:
            for half in range(2):
                ke.landed(half, *along(half, dz, dy))
    with jax.named_scope("q_start"):
        qe.start_straight(DIST[:1])
        for d in DIST:
            qe.start_bent(d)
        qe.start_straight(DIST[1:])
    with jax.named_scope("score0"):
        qx, bias = score_args(0)
        turn_step(qx=qx, bias=bias, weigh=False, blend=False)
    with jax.named_scope("turn2"):
        for dz, dy in UNITS[7:]:
            for half in range(2):
                turn(half, dz, dy)

    left, right, far = (wrap(place.x, n) * 2 + place.core for n in (3, 1, 2))
    top, low = pl.ds(0, D // 2), pl.ds(D // 2, D // 2)

    def ring(src, n, to):
        send(src, src, ws.at[n], wr.at[n], to)

    def weight_near():
        arrived(weight.at[left], wr.at[0])
        ring(weight.at[left, top], 3, place.at(1, 0, 0, 0))
        ring(weight.at[left], 4, place.at(0, 1, 0, 0))
        arrived(weight.at[right], wr.at[1])
        ring(weight.at[right, low], 5, place.at(3, 0, 0, 0))
        ring(weight.at[right], 6, place.at(0, 1, 0, 0))

    def weight_far():
        arrived(weight.at[far, top], wr.at[3])
        ring(weight.at[far, top], 7, place.at(0, 1, 0, 0))
        arrived(weight.at[far, low], wr.at[5])
        ring(weight.at[far, low], 8, place.at(0, 1, 0, 0))

    def give_back(u):
        dz, dy = unit_at(u)
        remote(
            osend.at[u], heads.at[u], os.at[u], orr.at[u], place.at(0, 0, back(dz), back(dy))
        ).start()

    def wait_unit(u):
        dz, dy = unit_at(u)
        arrived(qland.at[0, rows[0]], qrf.at[0, dy, dz])
        arrived(qland.at[0, rows[1]], qrf.at[1, dz, dy])

    def body(u, _):
        with jax.named_scope("q_wait"):
            wait_unit(u + 1)
        qx, bias = score_args(u + 1)
        osend[u - 1] = turn_step(qx=qx, bias=bias)
        return 0

    def body_send(u, _):
        give_back(u - 2)
        return body(u, _)

    with jax.named_scope("w_near"):
        weight_near()
    with jax.named_scope("first_unit"):
        wait_unit(1)
        qx, bias = score_args(1)
        turn_step(qx=qx, bias=bias, blend=False)
    lax.fori_loop(1, 3, body, 0)
    with jax.named_scope("passes"):
        for d in DIST:
            qe.pass_on(d)
    lax.fori_loop(3, 12, body_send, 0)
    with jax.named_scope("w_far"):
        weight_far()
    lax.fori_loop(12, NB - 1, body_send, 0)
    with jax.named_scope("last_units"):
        give_back(NB - 3)
        osend[NB - 2] = turn_step()
        osend[NB - 1] = turn_step(weigh=False)
        give_back(NB - 2)

    with jax.named_scope("w_wait"):
        for n in (2, 4, 6):
            arrived(weight.at[0], wr.at[n])
        for n in (7, 8):
            arrived(weight.at[0, top], wr.at[n])
    give_back(NB - 1)

    def fetch(units):
        for u in units:
            if u:
                arrived(osend.at[0], orr.at[u])
        for u in units:
            att[:, u * HD:(u + 1) * HD] = (heads if u else osend)[u].T

    def weight_rows(units, n):
        return jnp.concatenate(
            [weight[n, ds128(place.lon_at(*UNITS[u])), :] for u in units], axis=0
        )

    with jax.named_scope("fetch1"):
        fetch(range(EARLY))

    def first(n, _):
        for m in (2 * n, 2 * n + 1):
            partial[m] = jnp.dot(
                att[:, 0:EARLY * HD], weight_rows(range(EARLY), m), preferred_element_type=jnp.float32
            )
        return 0

    with jax.named_scope("proj1"):
        lax.fori_loop(0, 4, first, 0)
    with jax.named_scope("fetch2"):
        fetch(range(EARLY, NB))
    with jax.named_scope("proj2"):
        for n in range(8):
            out[:, n * 256:(n + 1) * 256] = (
                partial[n]
                + jnp.dot(
                    att[:, EARLY * HD:], weight_rows(range(EARLY, NB), n),
                    preferred_element_type=jnp.float32,
                )
            ).astype(jnp.bfloat16)
    with jax.named_scope("drain"):
        for e in (ke, ve, qe):
            e.sent()
        for c in started:
            c.wait_send()
        for u in range(1, NB):
            arrived(osend.at[0], os.at[u])


def per_device(queries, keys, values, partners, out_weight):
    hbm, vmem = pl.BlockSpec(memory_space=pltpu.HBM), pl.BlockSpec(memory_space=pltpu.VMEM)
    dma = pltpu.SemaphoreType.DMA
    bf16, f32 = jnp.bfloat16, jnp.float32
    return pl.pallas_call(
        kernel,
        out_shape=jax.ShapeDtypeStruct((BLK, D), bf16),
        in_specs=[hbm] * 4 + [vmem],
        out_specs=vmem,
        scratch_shapes=[
            pltpu.VMEM((3, BLK, D), bf16),
            pltpu.VMEM((NB, BLK, HD), bf16),
            pltpu.VMEM((NB, BLK, HD), bf16),
            pltpu.VMEM((NB, BLK, HD), bf16),
            pltpu.VMEM((NB, 1, SLOTS), jnp.int32),
            pltpu.VMEM((VR, NB * BLK), bf16),
            pltpu.VMEM((NB * BLK, BLK), f32),
            pltpu.VMEM((NB * BLK, BLK), bf16),
            pltpu.VMEM((NB, BLK), f32),
            pltpu.VMEM((NB, HD, BLK), bf16),
            pltpu.VMEM((NB, HD, BLK), bf16),
            pltpu.VMEM((BLK, D), bf16),
            pltpu.VMEM((8, BLK, 256), f32),
            pltpu.VMEM((8, D, 256), bf16),
            pltpu.VMEM((3, 2, 3, 3, HALF, HD), bf16),
        ]
        + [dma((2, 3)), dma((2, 3)), dma((2, 4, 4)), dma((2, 4, 4))] * 3
        + [dma((NB,)), dma((NB,)), dma((9,)), dma((9,)), dma((15,)), dma((15,)), dma((8,))],
        name="band_attention",
        compiler_params=pltpu.CompilerParams(
            collective_id=0, has_side_effects=True, vmem_limit_bytes=VMEM_MIB * 1024 * 1024
        ),
    )(queries, keys, values, out_weight, partners)


VMEM_MIB = 40


def solution(mesh):
    return jax.shard_map(
        per_device,
        mesh=mesh,
        in_specs=(
            P(("lat", "lon"), None),
            P(("lat", "lon"), None),
            P(("lat", "lon"), None),
            P(("lat", "lon"), None),
            P(None, "lat"),
        ),
        out_specs=P(("lat", "lon"), None),
        check_vma=False,
    )
```

```python
import math

import jax
import jax.numpy as jnp
from jax import lax
from jax.experimental import pallas as pl
from jax.experimental.pallas import tpu as pltpu
from jax.sharding import PartitionSpec as P

NB = 16
BLK = 256
HALF = BLK // 2
HD = 128
VR = 144
D = 2048
SCALE = math.log2(math.e) / math.sqrt(HD)
LOW = -1e30
SLOTS = 13


def split_q(q):
    x = q.astype(jnp.float32) * SCALE
    high = x.astype(jnp.bfloat16)
    low = (x - high.astype(jnp.float32)).astype(jnp.bfloat16)
    return jnp.concatenate([high, low], axis=1)


def bias_of(row, block, band_start):
    j = lax.broadcasted_iota(jnp.int32, (NB, SLOTS), 0)
    named = jnp.max(jnp.where(row == j + band_start, 1.0, 0.0), axis=1, keepdims=True)
    j = lax.broadcasted_iota(jnp.int32, (NB, BLK), 0)
    near = (j == block) | (j == lax.rem(block + 1, NB)) | (j == lax.rem(block + NB - 1, NB))
    return jnp.where(near, 0.0, jnp.where(named > 0.5, 0.0, LOW))


def step(s_ref, w_ref, sub_ref, vt_ref, k_ref, qx=None, bias=None, weigh=True, blend=True):
    best, total = None, None
    for j in range(NB):
        at = slice(j * BLK, (j + 1) * BLK)
        if blend:
            part = jnp.dot(vt_ref[:, at], w_ref[at, :], preferred_element_type=jnp.float32)
            total = part if total is None else total + part
        if weigh:
            less = sub_ref[j:j + 1, :]
            for r in range(j * BLK, (j + 1) * BLK, 16):
                w_ref[r:r + 16, :] = jnp.exp2(s_ref[r:r + 16, :] - less).astype(jnp.bfloat16)
        if qx is not None:
            keys = k_ref[j]
            s = lax.dot_general(
                jnp.concatenate([keys, keys], axis=1), qx, (((1,), (1,)), ((), ())),
                preferred_element_type=jnp.float32,
            )
            s_ref[at, :] = s
            part = jnp.max(s.reshape(BLK // 8, 8, BLK), axis=0) + bias[j:j + 1, :]
            best = part if best is None else jnp.maximum(best, part)
    if qx is not None:
        sub_ref[...] = jnp.max(best, axis=0, keepdims=True) - bias
    if blend:
        return (total[0:HD] / total[HD:HD + 1]).astype(jnp.bfloat16)
    return None


MESH = pl.DeviceIdType.MESH
DIST = (1, 3, 2)
RING = [(0, 0, dz, dy) for dz in range(4) for dy in range(4) if dz or dy]
EARLY = 12


def unit_at(u):
    four, seven = (u + 12) // 16, (u + 9) // 16
    dz = (four - seven) * (u - 3) + seven * ((u + 2) // 3 - 2)
    dy = (1 - four) * u + seven * ((u + 2) % 3 + 1)
    return dz, dy


UNITS = [unit_at(u) for u in range(NB)]


def wrap(a, d):
    return lax.rem(a + d, 4)


def back(d):
    return (4 - d) % 4


def ds128(i, n=1):
    return pl.ds(pl.multiple_of(i * 128, 128), n * 128)


class Place:
    def __init__(self):
        lat, lon = lax.axis_index("lat"), lax.axis_index("lon")
        self.x, self.core, self.z, self.y = lat // 2, lax.rem(lat, 2), lon // 4, lax.rem(lon, 4)
        self.lat, self.lon = lat, lon

    def at(self, dx, dc, dz, dy):
        return (
            wrap(self.x, dx) * 2 + lax.rem(self.core + dc, 2),
            wrap(self.z, dz) * 4 + wrap(self.y, dy),
        )

    def lon_at(self, dz, dy):
        return wrap(self.z, dz) * 4 + wrap(self.y, dy)


def remote(src, dst, ss, rs, to):
    return pltpu.make_async_remote_copy(
        src_ref=src, dst_ref=dst, send_sem=ss, recv_sem=rs, device_id=to, device_id_type=MESH
    )


def arrived(buf, sem):
    pltpu.make_async_copy(buf, buf, sem).wait()


def along(half, first, second):
    return (second, first) if half == 0 else (first, second)


class Exchange:
    def __init__(self, place, piece, landing, mid, final, sm, rm):
        self.place, self.piece, self.landing, self.mid = place, piece, landing, mid
        self.final, self.sm, self.rm = final, sm, rm

    def start_straight(self, distances=DIST):
        place = self.place
        for n in distances:
            for d, g in ((n, 0), (0, n)):
                for half in range(2):
                    o = along(half, d, g)
                    remote(
                        self.piece(half, place.lon_at(*o)), self.landing(half, d, g, place.lon),
                        self.sm, self.final(half, d, g), place.at(0, 0, *o),
                    ).start()

    def start_bent(self, d):
        place = self.place
        for g in DIST:
            for half in range(2):
                remote(
                    self.piece(half, place.lon_at(*along(half, d, g))), self.mid.at[half, d - 1, g - 1],
                    self.sm, self.rm.at[half, d - 1], place.at(0, 0, *along(half, d, 0)),
                ).start()

    def pass_on(self, d):
        place = self.place
        for half in range(2):
            arrived(self.mid.at[half, d - 1], self.rm.at[half, d - 1])
            block = place.lon_at(*along(half, back(d), 0))
            for g in DIST:
                remote(
                    self.mid.at[half, d - 1, g - 1], self.landing(half, d, g, block),
                    self.sm, self.final(half, d, g), place.at(0, 0, *along(half, 0, g)),
                ).start()

    def block_at(self, half, d, g):
        return self.place.lon_at(*along(half, back(d), back(g)))


def kernel(
    q, k, v, w, p, out,
    mine, kland, vland, qland, table, vt, sbuf, wbuf, sub, osend, heads, att, partial, weight, mid,
    krm, vrm, qrm, sent, klanded, vlanded, qlanded,
    orr, wr, ps, pr, lsem,
):
    place = Place()
    lat, lon = place.lat, place.lon
    band_start = lat * NB
    rows = (pl.ds(0, HALF), pl.ds(HALF, HALF))
    loads = [pltpu.make_async_copy(a, mine.at[n], lsem.at[n]) for n, a in enumerate((k, v, q))]
    for c in loads:
        c.start()
    local = [
        pltpu.make_async_copy(k.at[:, ds128(lon)], kland.at[lon], lsem.at[3]),
        pltpu.make_async_copy(v.at[:, ds128(lon)], vland.at[lon], lsem.at[4]),
        pltpu.make_async_copy(q.at[:, ds128(lon)], qland.at[0], lsem.at[5]),
        pltpu.make_async_copy(w, weight.at[lat], lsem.at[6]),
        pltpu.make_async_copy(p, table.at[lon], lsem.at[7]),
    ]
    for c in local:
        c.start()

    peers = RING + [(1, 0, 0, 0), (3, 0, 0, 0), (0, 1, 0, 0)]
    bar = pltpu.get_barrier_semaphore()
    with jax.named_scope("barrier"):
        for o in peers:
            pl.semaphore_signal(bar, inc=1, device_id=place.at(*o), device_id_type=MESH)
        pl.semaphore_wait(bar, len(peers))

    rows_sent = [
        remote(p, table.at[lon], ps.at[n], pr.at[n], place.at(*o)) for n, o in enumerate(RING)
    ]
    for c in rows_sent:
        c.start()

    def exchange(n, landing, final, rm):
        return Exchange(
            place, lambda half, head: mine.at[n, rows[half], ds128(head)], landing, mid.at[n],
            final, sent.at[n], rm,
        )

    def unit_of(half, d, g):
        return UNITS.index(along(half, d, g))

    ke = exchange(
        0, lambda half, d, g, b: kland.at[b, rows[half]], lambda half, d, g: klanded, krm
    )
    ve = exchange(
        1, lambda half, d, g, b: vland.at[b, rows[half]],
        lambda half, d, g: vlanded.at[1 if d and g else 0], vrm,
    )
    qe = exchange(
        2, lambda half, d, g, b: qland.at[unit_of(half, d, g), rows[half]],
        lambda half, d, g: qlanded.at[unit_of(half, d, g)], qrm,
    )
    def send_weight(src, dst, n, to):
        remote(src, dst, sent.at[3], wr.at[n], to).start()

    with jax.named_scope("starts"):
        for n, e in enumerate((ke, ve)):
            loads[n].wait()
            for d in DIST:
                e.start_bent(d)
            e.start_straight()
            if n == 0:
                send_weight(w, weight.at[lat], 0, place.at(1, 0, 0, 0))
                send_weight(w, weight.at[lat], 1, place.at(3, 0, 0, 0))
                send_weight(w, weight.at[lat], 2, place.at(0, 1, 0, 0))
        loads[2].wait()
    with jax.named_scope("k_pass"):
        for d in DIST:
            ke.pass_on(d)
    with jax.named_scope("v_pass"):
        for d in DIST:
            ve.pass_on(d)
        qe.start_straight()

    with jax.named_scope("table"):
        for c in local:
            c.wait()
        for n in range(len(RING)):
            arrived(table.at[0], pr.at[n])
        vt[HD:VR, :] = jnp.where(
            lax.broadcasted_iota(jnp.int32, (VR - HD, NB * BLK), 0) == 0, 1.0, 0.0
        ).astype(jnp.bfloat16)

    def turn(half, dz, dy):
        b = place.lon_at(back(dz), back(dy))
        vt[0:HD, ds128(2 * b + half)] = vland[b, rows[half]].T

    def score_args(u):
        dz, dy = unit_at(u)
        b = place.lon_at(back(dz), back(dy))
        return split_q(qland[u]), bias_of(table[b], b, band_start)

    def turn_step(**kwargs):
        return step(sbuf, wbuf, sub, vt, kland, **kwargs)

    def wait_unit(u):
        arrived(qland.at[0], qlanded.at[u])

    with jax.named_scope("turn1"):
        arrived(vland.at[0:6], vlanded.at[0])
        for half in range(2):
            for dz, dy in UNITS[:7]:
                turn(half, dz, dy)
    with jax.named_scope("k_wait"):
        arrived(kland.at[0:NB - 1], klanded)
    with jax.named_scope("q_start"):
        for d in DIST:
            qe.start_bent(d)
    with jax.named_scope("score0"):
        qx, bias = score_args(0)
        turn_step(qx=qx, bias=bias, weigh=False, blend=False)
    with jax.named_scope("turn2"):
        arrived(vland.at[0:9], vlanded.at[1])
        for dz, dy in UNITS[7:]:
            for half in range(2):
                turn(half, dz, dy)
    with jax.named_scope("first_unit"):
        wait_unit(1)
        qx, bias = score_args(1)
        turn_step(qx=qx, bias=bias, blend=False)

    left, right, far = (wrap(place.x, n) * 2 + place.core for n in (3, 1, 2))
    top, low = pl.ds(0, D // 2), pl.ds(D // 2, D // 2)

    def ring(src, n, to):
        send_weight(src, src, n, to)

    def weight_near():
        arrived(weight.at[left], wr.at[0])
        ring(weight.at[left, top], 3, place.at(1, 0, 0, 0))
        ring(weight.at[left], 4, place.at(0, 1, 0, 0))
        arrived(weight.at[right], wr.at[1])
        ring(weight.at[right, low], 5, place.at(3, 0, 0, 0))
        ring(weight.at[right], 6, place.at(0, 1, 0, 0))

    def weight_far():
        arrived(weight.at[far, top], wr.at[3])
        ring(weight.at[far, top], 7, place.at(0, 1, 0, 0))
        arrived(weight.at[far, low], wr.at[5])
        ring(weight.at[far, low], 8, place.at(0, 1, 0, 0))

    def give_back(u):
        dz, dy = unit_at(u)
        remote(
            osend.at[u], heads.at[u], sent.at[4], orr.at[(u + 4) // NB], place.at(0, 0, back(dz), back(dy))
        ).start()

    def body(u, _):
        with jax.named_scope("q_wait"):
            wait_unit(u + 1)
        qx, bias = score_args(u + 1)
        osend[u - 1] = turn_step(qx=qx, bias=bias)
        return 0

    def body_send(u, _):
        give_back(u - 2)
        return body(u, _)

    with jax.named_scope("w_near"):
        weight_near()
    lax.fori_loop(1, 3, body, 0)
    with jax.named_scope("passes"):
        for d in DIST:
            qe.pass_on(d)
    lax.fori_loop(3, 12, body_send, 0)
    with jax.named_scope("w_far"):
        weight_far()
    lax.fori_loop(12, NB - 1, body_send, 0)
    with jax.named_scope("last_units"):
        give_back(NB - 3)
        osend[NB - 2] = turn_step()
        osend[NB - 1] = turn_step(weigh=False)
        give_back(NB - 2)

    with jax.named_scope("w_wait"):
        for n in (2, 4, 6):
            arrived(weight.at[0], wr.at[n])
        for n in (7, 8):
            arrived(weight.at[0, top], wr.at[n])
    give_back(NB - 1)

    def fetch(units):
        late = units[0] // EARLY
        arrived(heads.at[0:(NB - EARLY if late else EARLY - 1)], orr.at[late])
        for u in units:
            att[:, u * HD:(u + 1) * HD] = (heads if u else osend)[u].T

    def weight_rows(units, n):
        return jnp.concatenate(
            [weight[n, ds128(place.lon_at(*UNITS[u])), :] for u in units], axis=0
        )

    with jax.named_scope("fetch1"):
        fetch(range(EARLY))

    def first(n, _):
        for m in (2 * n, 2 * n + 1):
            partial[m] = jnp.dot(
                att[:, 0:EARLY * HD], weight_rows(range(EARLY), m), preferred_element_type=jnp.float32
            )
        return 0

    with jax.named_scope("proj1"):
        lax.fori_loop(0, 4, first, 0)
    with jax.named_scope("fetch2"):
        fetch(range(EARLY, NB))
    with jax.named_scope("proj2"):
        for n in range(8):
            out[:, n * 256:(n + 1) * 256] = (
                partial[n]
                + jnp.dot(
                    att[:, EARLY * HD:], weight_rows(range(EARLY, NB), n),
                    preferred_element_type=jnp.float32,
                )
            ).astype(jnp.bfloat16)
    with jax.named_scope("drain"):
        for n in range(3):
            arrived(mine.at[:, 0:HALF], sent.at[n])
        arrived(weight.at[0:7], sent.at[3])
        arrived(osend.at[0:NB - 1], sent.at[4])
        for c in rows_sent:
            c.wait_send()


def per_device(queries, keys, values, partners, out_weight):
    hbm, vmem = pl.BlockSpec(memory_space=pltpu.HBM), pl.BlockSpec(memory_space=pltpu.VMEM)
    dma = pltpu.SemaphoreType.DMA
    bf16, f32 = jnp.bfloat16, jnp.float32
    return pl.pallas_call(
        kernel,
        out_shape=jax.ShapeDtypeStruct((BLK, D), bf16),
        in_specs=[hbm] * 4 + [vmem],
        out_specs=vmem,
        scratch_shapes=[
            pltpu.VMEM((3, BLK, D), bf16),
            pltpu.VMEM((NB, BLK, HD), bf16),
            pltpu.VMEM((NB, BLK, HD), bf16),
            pltpu.VMEM((NB, BLK, HD), bf16),
            pltpu.VMEM((NB, 1, SLOTS), jnp.int32),
            pltpu.VMEM((VR, NB * BLK), bf16),
            pltpu.VMEM((NB * BLK, BLK), f32),
            pltpu.VMEM((NB * BLK, BLK), bf16),
            pltpu.VMEM((NB, BLK), f32),
            pltpu.VMEM((NB, HD, BLK), bf16),
            pltpu.VMEM((NB, HD, BLK), bf16),
            pltpu.VMEM((BLK, D), bf16),
            pltpu.VMEM((8, BLK, 256), f32),
            pltpu.VMEM((8, D, 256), bf16),
            pltpu.VMEM((3, 2, 3, 3, HALF, HD), bf16),
        ]
        + [dma((2, 3))] * 3
        + [dma((5,)), dma, dma((2,)), dma((NB,))]
        + [dma((2,)), dma((9,)), dma((15,)), dma((15,)), dma((8,))],
        name="band_attention",
        compiler_params=pltpu.CompilerParams(
            collective_id=0, has_side_effects=True, vmem_limit_bytes=VMEM_MIB * 1024 * 1024
        ),
    )(queries, keys, values, out_weight, partners)


VMEM_MIB = 56


def solution(mesh):
    return jax.shard_map(
        per_device,
        mesh=mesh,
        in_specs=(
            P(("lat", "lon"), None),
            P(("lat", "lon"), None),
            P(("lat", "lon"), None),
            P(("lat", "lon"), None),
            P(None, "lat"),
        ),
        out_specs=P(("lat", "lon"), None),
        check_vma=False,
    )
```

```python
import math

import jax
import jax.numpy as jnp
from jax import lax
from jax.experimental import pallas as pl
from jax.experimental.pallas import tpu as pltpu
from jax.sharding import PartitionSpec as P

NB = 16
BLK = 256
HALF = BLK // 2
HD = 128
VR = 144
D = 2048
SCALE = math.log2(math.e) / math.sqrt(HD)
LOW = -1e30
SLOTS = 13


def split_q(q):
    x = q.astype(jnp.float32) * SCALE
    high = x.astype(jnp.bfloat16)
    low = (x - high.astype(jnp.float32)).astype(jnp.bfloat16)
    return jnp.concatenate([high, low], axis=1)


def bias_of(row, block, band_start):
    j = lax.broadcasted_iota(jnp.int32, (NB, SLOTS), 0)
    named = jnp.max(jnp.where(row == j + band_start, 1.0, 0.0), axis=1, keepdims=True)
    j = lax.broadcasted_iota(jnp.int32, (NB, BLK), 0)
    near = (j == block) | (j == lax.rem(block + 1, NB)) | (j == lax.rem(block + NB - 1, NB))
    return jnp.where(near, 0.0, jnp.where(named > 0.5, 0.0, LOW))


def step(s_ref, w_ref, sub_ref, vt_ref, k_ref, qx=None, bias=None, weigh=True, blend=True):
    best, total = None, None
    for j in range(NB):
        at = slice(j * BLK, (j + 1) * BLK)
        if blend:
            part = jnp.dot(vt_ref[:, at], w_ref[at, :], preferred_element_type=jnp.float32)
            total = part if total is None else total + part
        if weigh:
            less = sub_ref[j:j + 1, :]
            for r in range(j * BLK, (j + 1) * BLK, 16):
                w_ref[r:r + 16, :] = jnp.exp2(s_ref[r:r + 16, :] - less).astype(jnp.bfloat16)
        if qx is not None:
            keys = k_ref[j]
            s = lax.dot_general(
                jnp.concatenate([keys, keys], axis=1), qx, (((1,), (1,)), ((), ())),
                preferred_element_type=jnp.float32,
            )
            s_ref[at, :] = s
            part = jnp.max(s.reshape(BLK // 8, 8, BLK), axis=0) + bias[j:j + 1, :]
            best = part if best is None else jnp.maximum(best, part)
    if qx is not None:
        sub_ref[...] = jnp.max(best, axis=0, keepdims=True) - bias
    if blend:
        return (total[0:HD] / total[HD:HD + 1]).astype(jnp.bfloat16)
    return None


MESH = pl.DeviceIdType.MESH
DIST = (1, 3, 2)
RING = [(0, 0, dz, dy) for dz in range(4) for dy in range(4) if dz or dy]
EARLY = 12


def unit_at(u):
    four, seven = (u + 12) // 16, (u + 9) // 16
    dz = (four - seven) * (u - 3) + seven * ((u + 2) // 3 - 2)
    dy = (1 - four) * u + seven * ((u + 2) % 3 + 1)
    return dz, dy


UNITS = [unit_at(u) for u in range(NB)]


def wrap(a, d):
    return lax.rem(a + d, 4)


def back(d):
    return (4 - d) % 4


def ds128(i, n=1):
    return pl.ds(pl.multiple_of(i * 128, 128), n * 128)


class Place:
    def __init__(self):
        lat, lon = lax.axis_index("lat"), lax.axis_index("lon")
        self.x, self.core, self.z, self.y = lat // 2, lax.rem(lat, 2), lon // 4, lax.rem(lon, 4)
        self.lat, self.lon = lat, lon

    def at(self, dx, dc, dz, dy):
        return (
            wrap(self.x, dx) * 2 + lax.rem(self.core + dc, 2),
            wrap(self.z, dz) * 4 + wrap(self.y, dy),
        )

    def lon_at(self, dz, dy):
        return wrap(self.z, dz) * 4 + wrap(self.y, dy)


def remote(src, dst, ss, rs, to):
    return pltpu.make_async_remote_copy(
        src_ref=src, dst_ref=dst, send_sem=ss, recv_sem=rs, device_id=to, device_id_type=MESH
    )


def arrived(buf, sem):
    pltpu.make_async_copy(buf, buf, sem).wait()


def along(half, first, second):
    return (second, first) if half == 0 else (first, second)


class Exchange:
    def __init__(self, place, piece, landing, mid, final, sm, rm):
        self.place, self.piece, self.landing, self.mid = place, piece, landing, mid
        self.final, self.sm, self.rm = final, sm, rm

    def start_straight(self, distances=DIST):
        place = self.place
        for n in distances:
            for d, g in ((n, 0), (0, n)):
                for half in range(2):
                    o = along(half, d, g)
                    remote(
                        self.piece(half, place.lon_at(*o)), self.landing(half, d, g, place.lon),
                        self.sm, self.final(half, d, g), place.at(0, 0, *o),
                    ).start()

    def start_bent(self, d):
        place = self.place
        for g in DIST:
            for half in range(2):
                remote(
                    self.piece(half, place.lon_at(*along(half, d, g))), self.mid.at[half, d - 1, g - 1],
                    self.sm, self.rm.at[half, d - 1], place.at(0, 0, *along(half, d, 0)),
                ).start()

    def pass_on(self, d):
        place = self.place
        for half in range(2):
            arrived(self.mid.at[half, d - 1], self.rm.at[half, d - 1])
            block = place.lon_at(*along(half, back(d), 0))
            for g in DIST:
                remote(
                    self.mid.at[half, d - 1, g - 1], self.landing(half, d, g, block),
                    self.sm, self.final(half, d, g), place.at(0, 0, *along(half, 0, g)),
                ).start()

    def block_at(self, half, d, g):
        return self.place.lon_at(*along(half, back(d), back(g)))


def kernel(
    q, k, v, w, p, result,
    out, osem, mine, kland, vland, qland, table, vt, sbuf, wbuf, sub, osend, heads, att, partial, weight, mid,
    krm, vrm, qrm, sent, klanded, vlanded, qlanded,
    orr, wr, ps, pr, lsem,
):
    place = Place()
    lat, lon = place.lat, place.lon
    band_start = lat * NB
    rows = (pl.ds(0, HALF), pl.ds(HALF, HALF))
    loads = [pltpu.make_async_copy(a, mine.at[n], lsem.at[n]) for n, a in enumerate((k, v, q))]
    for c in loads:
        c.start()
    local = [
        pltpu.make_async_copy(k.at[:, ds128(lon)], kland.at[lon], lsem.at[3]),
        pltpu.make_async_copy(v.at[:, ds128(lon)], vland.at[lon], lsem.at[4]),
        pltpu.make_async_copy(q.at[:, ds128(lon)], qland.at[0], lsem.at[5]),
        pltpu.make_async_copy(w, weight.at[lat], lsem.at[6]),
        pltpu.make_async_copy(p, table.at[lon], lsem.at[7]),
    ]
    for c in local:
        c.start()

    peers = RING + [(1, 0, 0, 0), (3, 0, 0, 0), (0, 1, 0, 0)]
    bar = pltpu.get_barrier_semaphore()
    with jax.named_scope("barrier"):
        for o in peers:
            pl.semaphore_signal(bar, inc=1, device_id=place.at(*o), device_id_type=MESH)
        pl.semaphore_wait(bar, len(peers))

    rows_sent = [
        remote(p, table.at[lon], ps.at[n], pr.at[n], place.at(*o)) for n, o in enumerate(RING)
    ]
    for c in rows_sent:
        c.start()

    def exchange(n, landing, final, rm):
        return Exchange(
            place, lambda half, head: mine.at[n, rows[half], ds128(head)], landing, mid.at[n],
            final, sent.at[n], rm,
        )

    def unit_of(half, d, g):
        return UNITS.index(along(half, d, g))

    ke = exchange(
        0, lambda half, d, g, b: kland.at[b, rows[half]], lambda half, d, g: klanded, krm
    )
    ve = exchange(
        1, lambda half, d, g, b: vland.at[b, rows[half]],
        lambda half, d, g: vlanded.at[1 if d and g else 0], vrm,
    )
    qe = exchange(
        2, lambda half, d, g, b: qland.at[unit_of(half, d, g), rows[half]],
        lambda half, d, g: qlanded.at[unit_of(half, d, g)], qrm,
    )
    def send_weight(src, dst, n, to):
        remote(src, dst, sent.at[3], wr.at[n], to).start()

    with jax.named_scope("starts"):
        for n, e in enumerate((ke, ve)):
            loads[n].wait()
            for d in DIST:
                e.start_bent(d)
            e.start_straight()
            if n == 0:
                send_weight(w, weight.at[lat], 0, place.at(1, 0, 0, 0))
                send_weight(w, weight.at[lat], 1, place.at(3, 0, 0, 0))
                send_weight(w, weight.at[lat], 2, place.at(0, 1, 0, 0))
        loads[2].wait()
    with jax.named_scope("k_pass"):
        for d in DIST:
            ke.pass_on(d)
    with jax.named_scope("v_pass"):
        for d in DIST:
            ve.pass_on(d)
        qe.start_straight()

    with jax.named_scope("table"):
        for c in local:
            c.wait()
        for n in range(len(RING)):
            arrived(table.at[0], pr.at[n])
        vt[HD:VR, :] = jnp.where(
            lax.broadcasted_iota(jnp.int32, (VR - HD, NB * BLK), 0) == 0, 1.0, 0.0
        ).astype(jnp.bfloat16)

    def turn(half, dz, dy):
        b = place.lon_at(back(dz), back(dy))
        vt[0:HD, ds128(2 * b + half)] = vland[b, rows[half]].T

    def score_args(u):
        dz, dy = unit_at(u)
        b = place.lon_at(back(dz), back(dy))
        return split_q(qland[u]), bias_of(table[b], b, band_start)

    def turn_step(**kwargs):
        return step(sbuf, wbuf, sub, vt, kland, **kwargs)

    def wait_unit(u):
        arrived(qland.at[0], qlanded.at[u])

    with jax.named_scope("turn1"):
        arrived(vland.at[0:6], vlanded.at[0])
        for half in range(2):
            for dz, dy in UNITS[:7]:
                turn(half, dz, dy)
    with jax.named_scope("k_wait"):
        arrived(kland.at[0:NB - 1], klanded)
    with jax.named_scope("q_start"):
        for d in DIST:
            qe.start_bent(d)
    with jax.named_scope("score0"):
        qx, bias = score_args(0)
        turn_step(qx=qx, bias=bias, weigh=False, blend=False)
    with jax.named_scope("turn2"):
        arrived(vland.at[0:9], vlanded.at[1])
        for dz, dy in UNITS[7:]:
            for half in range(2):
                turn(half, dz, dy)
    with jax.named_scope("first_unit"):
        wait_unit(1)
        qx, bias = score_args(1)
        turn_step(qx=qx, bias=bias, blend=False)

    left, right, far = (wrap(place.x, n) * 2 + place.core for n in (3, 1, 2))
    top, low = pl.ds(0, D // 2), pl.ds(D // 2, D // 2)

    def ring(src, n, to):
        send_weight(src, src, n, to)

    def weight_near():
        arrived(weight.at[left], wr.at[0])
        ring(weight.at[left, top], 3, place.at(1, 0, 0, 0))
        ring(weight.at[left], 4, place.at(0, 1, 0, 0))
        arrived(weight.at[right], wr.at[1])
        ring(weight.at[right, low], 5, place.at(3, 0, 0, 0))
        ring(weight.at[right], 6, place.at(0, 1, 0, 0))

    def weight_far():
        arrived(weight.at[far, top], wr.at[3])
        ring(weight.at[far, top], 7, place.at(0, 1, 0, 0))
        arrived(weight.at[far, low], wr.at[5])
        ring(weight.at[far, low], 8, place.at(0, 1, 0, 0))

    def give_back(u):
        dz, dy = unit_at(u)
        remote(
            osend.at[u], heads.at[u], sent.at[4], orr.at[(u + 4) // NB], place.at(0, 0, back(dz), back(dy))
        ).start()

    def body(u, _):
        with jax.named_scope("q_wait"):
            wait_unit(u + 1)
        qx, bias = score_args(u + 1)
        osend[u - 1] = turn_step(qx=qx, bias=bias)
        return 0

    def body_send(u, _):
        give_back(u - 2)
        return body(u, _)

    with jax.named_scope("w_near"):
        weight_near()
    lax.fori_loop(1, 3, body, 0)
    with jax.named_scope("passes"):
        for d in DIST:
            qe.pass_on(d)
    lax.fori_loop(3, 12, body_send, 0)
    with jax.named_scope("w_far"):
        weight_far()
    lax.fori_loop(12, NB - 1, body_send, 0)
    with jax.named_scope("last_units"):
        give_back(NB - 3)
        osend[NB - 2] = turn_step()
        osend[NB - 1] = turn_step(weigh=False)
        give_back(NB - 2)

    with jax.named_scope("w_wait"):
        for n in (2, 4, 6):
            arrived(weight.at[0], wr.at[n])
        for n in (7, 8):
            arrived(weight.at[0, top], wr.at[n])
    give_back(NB - 1)

    def fetch(units):
        late = units[0] // EARLY
        arrived(heads.at[0:(NB - EARLY if late else EARLY - 1)], orr.at[late])
        for u in units:
            att[:, u * HD:(u + 1) * HD] = (heads if u else osend)[u].T

    def weight_rows(units, n):
        return jnp.concatenate(
            [weight[n, ds128(place.lon_at(*UNITS[u])), :] for u in units], axis=0
        )

    with jax.named_scope("fetch1"):
        fetch(range(EARLY))

    def first(n, _):
        for m in (2 * n, 2 * n + 1):
            partial[m] = jnp.dot(
                att[:, 0:EARLY * HD], weight_rows(range(EARLY), m), preferred_element_type=jnp.float32
            )
        return 0

    with jax.named_scope("proj1"):
        lax.fori_loop(0, 4, first, 0)
    with jax.named_scope("fetch2"):
        fetch(range(EARLY, NB))
    def put(n):
        tile = pl.ds(n * 256, 256)
        return pltpu.make_async_copy(out.at[:, tile], result.at[:, tile], osem.at[n])

    with jax.named_scope("proj2"):
        for n in range(8):
            out[:, n * 256:(n + 1) * 256] = (
                partial[n]
                + jnp.dot(
                    att[:, EARLY * HD:], weight_rows(range(EARLY, NB), n),
                    preferred_element_type=jnp.float32,
                )
            ).astype(jnp.bfloat16)
            put(n).start()
    with jax.named_scope("drain"):
        for n in range(8):
            put(n).wait()
        for n in range(3):
            arrived(mine.at[:, 0:HALF], sent.at[n])
        arrived(weight.at[0:7], sent.at[3])
        arrived(osend.at[0:NB - 1], sent.at[4])
        for c in rows_sent:
            c.wait_send()


def per_device(queries, keys, values, partners, out_weight):
    hbm, vmem = pl.BlockSpec(memory_space=pltpu.HBM), pl.BlockSpec(memory_space=pltpu.VMEM)
    dma = pltpu.SemaphoreType.DMA
    bf16, f32 = jnp.bfloat16, jnp.float32
    return pl.pallas_call(
        kernel,
        out_shape=jax.ShapeDtypeStruct((BLK, D), bf16),
        in_specs=[hbm] * 4 + [vmem],
        out_specs=hbm,
        scratch_shapes=[
            pltpu.VMEM((BLK, D), bf16),
            dma((8,)),
            pltpu.VMEM((3, BLK, D), bf16),
            pltpu.VMEM((NB, BLK, HD), bf16),
            pltpu.VMEM((NB, BLK, HD), bf16),
            pltpu.VMEM((NB, BLK, HD), bf16),
            pltpu.VMEM((NB, 1, SLOTS), jnp.int32),
            pltpu.VMEM((VR, NB * BLK), bf16),
            pltpu.VMEM((NB * BLK, BLK), f32),
            pltpu.VMEM((NB * BLK, BLK), bf16),
            pltpu.VMEM((NB, BLK), f32),
            pltpu.VMEM((NB, HD, BLK), bf16),
            pltpu.VMEM((NB, HD, BLK), bf16),
            pltpu.VMEM((BLK, D), bf16),
            pltpu.VMEM((8, BLK, 256), f32),
            pltpu.VMEM((8, D, 256), bf16),
            pltpu.VMEM((3, 2, 3, 3, HALF, HD), bf16),
        ]
        + [dma((2, 3))] * 3
        + [dma((5,)), dma, dma((2,)), dma((NB,))]
        + [dma((2,)), dma((9,)), dma((15,)), dma((15,)), dma((8,))],
        name="band_attention",
        compiler_params=pltpu.CompilerParams(
            collective_id=0, has_side_effects=True, vmem_limit_bytes=VMEM_MIB * 1024 * 1024
        ),
    )(queries, keys, values, out_weight, partners)


VMEM_MIB = 56


def solution(mesh):
    return jax.shard_map(
        per_device,
        mesh=mesh,
        in_specs=(
            P(("lat", "lon"), None),
            P(("lat", "lon"), None),
            P(("lat", "lon"), None),
            P(("lat", "lon"), None),
            P(None, "lat"),
        ),
        out_specs=P(("lat", "lon"), None),
        check_vma=False,
    )
```
